32 devices in a mesh: ta: 2 (over x), ha: 4 (over y, core), wa: 4 (over z).
Axes of the slice: x: 2, y: 2, z: 4, core: 2. Of those that a mesh axis runs over, the one named last changes fastest.
Arguments:
- volume: bfloat16 [2, 128, 64, 128], P('ta', 'ha', 'wa'), may hold values from -6 to 6
- cotangent: bfloat16 [2, 128, 64, 128], P('ta', 'ha', 'wa'), may hold values from -6 to 6
- kernel_one: bfloat16 [3, 3, 3, 128, 128], replicated, may hold values from -0.109375 to 0.109375
- kernel_two: bfloat16 [3, 3, 3, 128, 128], replicated, may hold values from -0.109375 to 0.109375
Outputs:
- d_volume: bfloat16 [2, 128, 64, 128], P('ta', 'ha', 'wa')
- grad_one: float32 [3, 3, 3, 128, 128], replicated
- grad_two: float32 [3, 3, 3, 128, 128], replicated
The draws below stay inside these ranges and needn't reach their ends.
All inputs are finite; a program needn't handle non-finite values.
Results may differ from the reference program's by a relative error of at most 0.0049.
Values may be sent and summed in bfloat16 or wider, within the bound.
No kernel may reach another device: no remote copies, remote signals or barrier semaphores. Data moves between devices by JAX's collectives and lax.ppermute only.
A program may use at most 64 MiB of HBM per device.

```python
import jax
import jax.numpy as jnp
from jax import lax

CHANNELS = 128
FRAMES = 2
HEIGHT = 128
WIDTH_ALL = 64


def steps_of(rng, dims, shards, smallest, high):
    gain, own = 1.0, jax.random.fold_in(rng, 6)
    for dim, blocks in shards:
        draws = jnp.exp(jax.random.uniform(jax.random.fold_in(own, dim), (blocks,), jnp.float32, smallest / len(shards), high / len(shards)))
        gain = gain * jnp.repeat(draws, dims[dim] // blocks).reshape([-1 if axis == dim else 1 for axis in range(len(dims))])
    return gain


def centred(own_key, extent, spread, reach, split=(), dtype=jnp.bfloat16):
    array = spread * jax.random.normal(own_key, extent, jnp.float32)
    if split:
        array = array * steps_of(own_key, extent, split, -0.22, 0.18)
    return jnp.clip(array, -reach, reach).astype(dtype)


def setup_inputs(seed: int = 0) -> dict:
    splits = jax.random.split(jax.random.key(seed), 5)
    volume = centred(splits[0], (FRAMES, HEIGHT, WIDTH_ALL, CHANNELS), 1.0, 6.0, ((0, 2), (1, 4), (2, 4)))
    cotangent = centred(splits[1], (FRAMES, HEIGHT, WIDTH_ALL, CHANNELS), 1.0, 6.0, ((0, 2), (1, 4), (2, 4)))
    kernel_one = centred(splits[2], (3, 3, 3, CHANNELS, CHANNELS), (27 * CHANNELS) ** -0.5, 0.109375)
    kernel_two = centred(splits[3], (3, 3, 3, CHANNELS, CHANNELS), (27 * CHANNELS) ** -0.5, 0.109375)
    return {"volume": volume, "cotangent": cotangent, "kernel_one": kernel_one, "kernel_two": kernel_two}


def flip_swap(kernel):
    return jnp.swapaxes(kernel[::-1, ::-1, ::-1], 3, 4)

def pad_field(field):
    return jnp.pad(field.astype(jnp.float32), ((1, 1), (1, 1), (1, 1), (0, 0)))

def conv_full(field, kernel):
    frames, height, width, chans = field.shape
    padded = pad_field(field)
    total = jnp.zeros((frames * height * width, chans), jnp.float32)
    for kt in range(3):
        for kh in range(3):
            for kw in range(3):
                piece = padded[kt:kt + frames, kh:kh + height, kw:kw + width].reshape(-1, chans)
                total = total + jnp.dot(piece, kernel[kt, kh, kw].astype(jnp.float32), precision=lax.Precision.HIGHEST)
    return total.reshape(frames, height, width, chans)

def kernel_grad(field, other):
    frames, height, width, chans = field.shape
    padded = pad_field(field)
    right = other.astype(jnp.float32).reshape(-1, chans)
    blocks = []
    for kt in range(3):
        for kh in range(3):
            for kw in range(3):
                piece = padded[kt:kt + frames, kh:kh + height, kw:kw + width].reshape(-1, chans)
                blocks.append(jnp.dot(piece.T, right, precision=lax.Precision.HIGHEST))
    return jnp.stack(blocks).reshape(3, 3, 3, chans, chans)

def reference(volume, cotangent, kernel_one, kernel_two):
    pre = conv_full(volume, kernel_one)
    sig = jax.nn.sigmoid(pre)
    hidden = (pre * sig).astype(jnp.bfloat16)
    d_hidden = conv_full(cotangent, flip_swap(kernel_two))
    d_pre = (d_hidden * sig * (1.0 + pre * (1.0 - sig))).astype(jnp.bfloat16)
    d_volume = conv_full(d_pre, flip_swap(kernel_one)).astype(jnp.bfloat16)
    scale = 1.0 / jnp.sqrt(jnp.float32(FRAMES * HEIGHT * WIDTH_ALL))
    grad_two = kernel_grad(hidden, cotangent) * scale
    grad_one = kernel_grad(volume, d_pre) * scale
    return (d_volume, grad_one, grad_two)
```

```python
import functools
import math

import jax
import jax.numpy as jnp
from jax import lax
from jax.experimental import pallas as pl
from jax.experimental.pallas import tpu as pltpu
from jax.sharding import PartitionSpec as P

AXES = ("ta", "ha", "wa")
BF16 = jnp.bfloat16
F32 = jnp.float32


def both_ways(array_down, array_up, axis):
    count = lax.axis_size(axis)
    down = lax.ppermute(array_down, axis, [(i, i + 1) for i in range(count - 1)])
    up = lax.ppermute(array_up, axis, [(i + 1, i) for i in range(count - 1)])
    return down, up


def halo(cells):
    prev, nxt = both_ways(cells[:, -1:], cells[:, :1], "ta")
    left, right = both_ways(cells[:, :, :, -1], cells[:, :, :, 0], "wa")
    row_first = jnp.concatenate([cells[:, :, 0], left[:, :, :1], right[:, :, :1]], axis=2)
    row_last = jnp.concatenate([cells[:, :, -1], left[:, :, -1:], right[:, :, -1:]], axis=2)
    above, below = both_ways(row_last, row_first, "ha")
    width = cells.shape[3]
    rim = jnp.concatenate(
        [
            above[:, :, :width],
            below[:, :, :width],
            above[:, :, width : width + 1],
            left,
            below[:, :, width : width + 1],
            above[:, :, width + 1 :],
            right,
            below[:, :, width + 1 :],
        ],
        axis=2,
    )
    rim_prev, rim_next = both_ways(rim[:, -1:], rim[:, :1], "ta")
    return prev, nxt, rim, rim_prev, rim_next


def fill_frame(rows, slot, cells, cells_at, rim, rim_at, height, width):
    chans = rows.shape[-1] // 3
    place = lax.broadcasted_iota(jnp.int32, (width, chans), 0)
    edge = 2 * width
    for h in range(height + 2):
        if h == 0:
            tile = rim[rim_at + (slice(0, width),)].astype(F32)
        elif h == height + 1:
            tile = rim[rim_at + (slice(width, 2 * width),)].astype(F32)
        else:
            tile = cells[cells_at + (h - 1,)].astype(F32)
        left = rim[rim_at + (slice(edge + h, edge + h + 1),)]
        right = rim[rim_at + (slice(edge + height + 2 + h, edge + height + 3 + h),)]
        before = jnp.where(place == 0, left, pltpu.roll(tile, 1, axis=0))
        after = jnp.where(place == width - 1, right, pltpu.roll(tile, width - 1, axis=0))
        span = slice(h * width, (h + 1) * width)
        rows[slot, span, 0:chans] = before.astype(BF16)
        rows[slot, span, chans : 2 * chans] = tile.astype(BF16)
        rows[slot, span, 2 * chans :] = after.astype(BF16)


def conv_rows(rows, weights, frame, height, width):
    total = None
    for kt in range(3):
        for kh in range(3):
            part = jnp.dot(
                rows[frame + kt, kh * width : (kh + height) * width, :],
                weights[kt * 3 + kh],
                preferred_element_type=F32,
            )
            total = part if total is None else total + part
    return total


def front_kernel(
    mine, vol, cot, prev, nxt, rim, rim_prev, rim_next, w_one, w_two,
    d_pre_out, keep, send, vol_rows, cot_rows, own_f, prev_f, next_f, grads,
):
    frames, height, width, chans = vol.shape
    own_f[...] = rim[...].astype(F32)
    prev_f[...] = rim_prev[...].astype(F32)
    next_f[...] = rim_next[...].astype(F32)
    for field, (rows, cells) in enumerate(((vol_rows, vol), (cot_rows, cot))):
        fill_frame(rows, 0, prev, (field, 0), prev_f, (field, 0), height, width)
        for t in range(frames):
            fill_frame(rows, t + 1, cells, (t,), own_f, (field, t), height, width)
        fill_frame(rows, frames + 1, nxt, (field, 0), next_f, (field, 0), height, width)
    for t in range(frames):
        pre = conv_rows(vol_rows, w_one, t, height, width)
        d_hidden = conv_rows(cot_rows, w_two, t, height, width)
        sig = 1.0 / (1.0 + jnp.exp(-pre))
        hidden_t = (pre * sig).T.astype(BF16)
        d_pre = (d_hidden * sig * (1.0 + pre * (1.0 - sig))).astype(BF16)
        d_pre_out[t] = d_pre.reshape(height, width, chans)
        for kt in range(3):
            for kh in range(3):
                span = slice(kh * width, (kh + height) * width)
                one = lax.dot_general(
                    vol_rows[t + kt, span, :], d_pre, (((0,), (0,)), ((), ())), preferred_element_type=F32
                )
                two = jnp.dot(hidden_t, cot_rows[t + kt, span, :], preferred_element_type=F32)
                at_one = slice((kt * 3 + kh) * 3 * chans, (kt * 3 + kh + 1) * 3 * chans)
                grads[0, at_one, :] = one if t == 0 else grads[0, at_one, :] + one
                for kw in range(3):
                    block = 26 - (kt * 9 + kh * 3 + kw)
                    at_two = slice(block * chans, (block + 1) * chans)
                    piece = two[:, kw * chans : (kw + 1) * chans]
                    grads[1, at_two, :] = piece if t == 0 else grads[1, at_two, :] + piece
    keep[...] = grads[mine[0]]
    send[...] = grads[1 - mine[0]].astype(BF16)


def back_kernel(cells, prev, nxt, rim, rim_prev, rim_next, weights, out, rows, own_f, prev_f, next_f):
    _, frames, height, width, chans = cells.shape
    own_f[...] = rim[...].astype(F32)
    prev_f[...] = rim_prev[...].astype(F32)
    next_f[...] = rim_next[...].astype(F32)
    fill_frame(rows, 0, prev, (0, 0), prev_f, (0, 0), height, width)
    for t in range(frames):
        fill_frame(rows, t + 1, cells, (0, t), own_f, (0, t), height, width)
    fill_frame(rows, frames + 1, nxt, (0, 0), next_f, (0, 0), height, width)
    for t in range(frames):
        total = conv_rows(rows, weights, t, height, width)
        out[t] = total.astype(BF16).reshape(height, width, chans)


def share_kernel(count, mine, own, *refs):
    received, outs = refs[: len(refs) - count], refs[len(refs) - count :]
    for other in range(count):
        chunk = mine[0] ^ other
        total = own[chunk]
        for part in received:
            total = total + part[chunk].astype(F32)
        outs[other][...] = total.astype(outs[other].dtype)


def merge_kernel(count, inner, places, *refs):
    mine, other, (first, second) = refs[:count], refs[count : 2 * count], refs[2 * count :]
    is_first = places[0] == 0
    for far in range(count):
        for near in range(inner):
            at = (places[1] ^ far) * inner + (places[2] ^ near)
            here = mine[far][near].astype(F32)
            there = other[far][near].astype(F32)
            first[at] = jnp.where(is_first, here, there)
            second[at] = jnp.where(is_first, there, here)


VMEM = pl.BlockSpec(memory_space=pltpu.VMEM)
SMEM = pl.BlockSpec(memory_space=pltpu.SMEM)


def call(kernel, outs, scalars, arrays, scratch=(), name=None):
    return pl.pallas_call(
        kernel,
        out_shape=outs,
        in_specs=[SMEM] * len(scalars) + [VMEM] * len(arrays),
        out_specs=jax.tree.map(lambda _: VMEM, outs),
        scratch_shapes=list(scratch),
        name=name,
    )(*scalars, *arrays)


def shape(dims, dtype):
    return jax.ShapeDtypeStruct(tuple(dims), dtype)


def swap_with(array, mask, devices):
    return lax.ppermute(array, AXES, [(d, d ^ mask) for d in range(devices)])


def flip_swap(kernel):
    return jnp.swapaxes(kernel[::-1, ::-1, ::-1], 3, 4)


def body(volume, cotangent, kernel_one, kernel_two):
    frames, height, width, chans = volume.shape
    sizes = {axis: lax.axis_size(axis) for axis in AXES}
    devices = math.prod(sizes.values())
    bits_w, bits_h, bits_t = (sizes[axis].bit_length() - 1 for axis in ("wa", "ha", "ta"))
    pair_bit = bits_w
    far_bits = [bits_w + k for k in range(1, bits_h + bits_t)]
    near_bits = list(range(bits_w))
    here = lax.axis_index(AXES)

    def part_of(bits):
        place = jnp.zeros((), jnp.int32)
        for k, bit in enumerate(bits):
            place = place | (((here >> bit) & 1) << k)
        return place

    def mask_of(bits, number):
        return sum(1 << bit for k, bit in enumerate(bits) if (number >> k) & 1)

    pair, far, near = part_of([pair_bit]), part_of(far_bits), part_of(near_bits)
    far_count, near_count = 1 << len(far_bits), 1 << len(near_bits)

    w_one = kernel_one.reshape(9, 3 * chans, chans)
    w_two = flip_swap(kernel_two).reshape(9, 3 * chans, chans)
    w_back = flip_swap(kernel_one).reshape(9, 3 * chans, chans)

    around = halo(jnp.stack((volume, cotangent)))
    rim_rows = 2 * width + 2 * (height + 2)
    patch = pltpu.VMEM((frames + 2, (height + 2) * width, 3 * chans), BF16)
    total_rows = 27 * chans
    d_pre, keep, send = call(
        front_kernel,
        (
            shape(volume.shape, BF16),
            shape((total_rows, chans), F32),
            shape((total_rows, chans), BF16),
        ),
        (pair.reshape(1),),
        (volume, cotangent, *around, w_one, w_two),
        (
            patch,
            patch,
            pltpu.VMEM((2, frames, rim_rows, chans), F32),
            pltpu.VMEM((2, 1, rim_rows, chans), F32),
            pltpu.VMEM((2, 1, rim_rows, chans), F32),
            pltpu.VMEM((2, total_rows, chans), F32),
        ),
        name="front",
    )

    def spread(place, own, received, bits):
        count = 1 << len(bits)
        rows = own.shape[0] // count
        split = lambda array: array.reshape(count, rows, chans)
        own, *sends = call(
            functools.partial(share_kernel, count),
            [shape((rows, chans), F32)] + [shape((rows, chans), BF16)] * (count - 1),
            (place.reshape(1),),
            [split(own)] + [split(part) for part in received],
            name="share",
        )
        return own, [swap_with(part, mask_of(bits, m + 1), devices) for m, part in enumerate(sends)]

    from_pair = swap_with(send, 1 << pair_bit, devices)
    own, received = spread(far, keep, [from_pair], far_bits)
    own, received = spread(near, own, received, near_bits)
    scale = 1.0 / jnp.sqrt(F32(frames * height * width * devices))
    for part in received:
        own = own + part.astype(F32)
    own = (own * scale).astype(BF16)

    block = jnp.stack([own] + [swap_with(own, mask_of(near_bits, m), devices) for m in range(1, near_count)])
    blocks = [block] + [swap_with(block, mask_of(far_bits, m), devices) for m in range(1, far_count)]
    others = [swap_with(part, 1 << pair_bit, devices) for part in blocks]

    around = halo(d_pre[None])
    d_volume = call(
        back_kernel,
        shape(volume.shape, BF16),
        (),
        (d_pre[None], *around, w_back),
        (
            patch,
            pltpu.VMEM((1, frames, rim_rows, chans), F32),
            pltpu.VMEM((1, 1, rim_rows, chans), F32),
            pltpu.VMEM((1, 1, rim_rows, chans), F32),
        ),
        name="back",
    )
    grad_shape = shape((far_count * near_count, own.shape[0], chans), F32)
    grad_one, grad_two = call(
        functools.partial(merge_kernel, far_count, near_count),
        (grad_shape, grad_shape),
        (jnp.stack((pair, far, near)),),
        (*blocks, *others),
        name="merge",
    )
    return d_volume, grad_one.reshape(kernel_one.shape), grad_two.reshape(kernel_two.shape)


def solution(mesh):
    spec = P("ta", "ha", "wa", None)
    return jax.shard_map(
        body, mesh=mesh, in_specs=(spec, spec, P(), P()), out_specs=(spec, P(), P()), check_vma=False
    )
```

```python
import functools
import math

import jax
import jax.numpy as jnp
from jax import lax
from jax.experimental import pallas as pl
from jax.experimental.pallas import tpu as pltpu
from jax.sharding import PartitionSpec as P

AXES = ("ta", "ha", "wa")
BF16 = jnp.bfloat16
F32 = jnp.float32
VMEM_LIMIT = 24 << 20


def both_ways(array_down, array_up, axis):
    count = lax.axis_size(axis)
    if count == 2 and array_down is array_up:
        other = lax.ppermute(array_down, axis, [(0, 1), (1, 0)])
        return other, other
    down = lax.ppermute(array_down, axis, [(i, (i + 1) % count) for i in range(count)])
    up = lax.ppermute(array_up, axis, [((i + 1) % count, i) for i in range(count)])
    return down, up


def frame_edges(cells):
    if cells.shape[1] == 1:
        return cells, cells
    return cells[:, -1:], cells[:, :1]


def column_halo(cells):
    return both_ways(cells[:, :, :, -1], cells[:, :, :, 0], "wa")


def row_halo(cells, left, right):
    width = cells.shape[3]
    zeros = jnp.zeros(cells.shape[:2] + (width - 2, cells.shape[4]), cells.dtype)
    row_first = jnp.concatenate([cells[:, :, 0], left[:, :, :1], right[:, :, :1], zeros], axis=2)
    row_last = jnp.concatenate([cells[:, :, -1], left[:, :, -1:], right[:, :, -1:], zeros], axis=2)
    return both_ways(row_last, row_first, "ha")


def rim_of(above, below, left, right):
    return jnp.concatenate([left, right, above, below], axis=2)


def load_rim(target, rim, live, inside, height, width):
    top, low = 2 * height, 2 * height + 2 * width
    row = lax.broadcasted_iota(jnp.int32, rim.shape[-2:], 0)
    above = (row >= top) & (row < low)
    below = row >= low
    left = (row < height) | (row == top + width) | (row == low + width)
    right = ((row >= height) & (row < top)) | (row == top + width + 1) | (row == low + width + 1)
    ok = jnp.where(above, inside[3], 1) * jnp.where(below, inside[4], 1)
    ok = ok * jnp.where(left, inside[5], 1) * jnp.where(right, inside[6], 1) * live
    for f in range(rim.shape[0]):
        for t in range(rim.shape[1]):
            target[f, t] = jnp.where(ok != 0, rim[f, t].astype(F32), 0.0)


def fill_frame(rows, slot, cells, cells_at, rim, rim_at, height, width, live=None):
    chans = rows.shape[-1] // 3
    place = lax.broadcasted_iota(jnp.int32, (width, chans), 0)
    top, low = 2 * height, 2 * height + 2 * width
    for h in range(height + 2):
        if h == 0:
            tile = rim[rim_at + (slice(top, top + width),)].astype(F32)
        elif h == height + 1:
            tile = rim[rim_at + (slice(low, low + width),)].astype(F32)
        else:
            tile = cells[cells_at + (h - 1,)].astype(F32)
            if live is not None:
                tile = jnp.where(live != 0, tile, 0.0)
        at_left, at_right = h - 1, height + h - 1
        if h == 0:
            at_left, at_right = top + width, top + width + 1
        elif h == height + 1:
            at_left, at_right = low + width, low + width + 1
        left = rim[rim_at + (slice(at_left, at_left + 1),)]
        right = rim[rim_at + (slice(at_right, at_right + 1),)]
        before = jnp.where(place == 0, left, pltpu.roll(tile, 1, axis=0))
        after = jnp.where(place == width - 1, right, pltpu.roll(tile, width - 1, axis=0))
        span = slice(h * width, (h + 1) * width)
        rows[slot, span, 0:chans] = before.astype(BF16)
        rows[slot, span, chans : 2 * chans] = tile.astype(BF16)
        rows[slot, span, 2 * chans :] = after.astype(BF16)


def conv_rows(rows, weights, frame, height, width):
    total = None
    for kt in range(3):
        for kh in range(3):
            part = jnp.dot(
                rows[frame + kt, kh * width : (kh + height) * width, :],
                weights[kt * 3 + kh],
                preferred_element_type=F32,
            )
            total = part if total is None else total + part
    return total


def front_kernel(
    mine, vol, cot, prev, nxt, rim, rim_prev, rim_next, w_one, w_two,
    d_pre_out, keep, send, vol_rows, cot_rows, own_f, prev_f, next_f, grads,
):
    frames, height, width, chans = vol.shape
    load_rim(own_f, rim, 1, mine, height, width)
    load_rim(prev_f, rim_prev, mine[1], mine, height, width)
    load_rim(next_f, rim_next, mine[2], mine, height, width)
    for field, (rows, cells) in enumerate(((vol_rows, vol), (cot_rows, cot))):
        fill_frame(rows, 0, prev, (field, 0), prev_f, (field, 0), height, width, mine[1])
        for t in range(frames):
            fill_frame(rows, t + 1, cells, (t,), own_f, (field, t), height, width)
        fill_frame(rows, frames + 1, nxt, (field, 0), next_f, (field, 0), height, width, mine[2])
    for t in range(frames):
        pre = conv_rows(vol_rows, w_one, t, height, width)
        d_hidden = conv_rows(cot_rows, w_two, t, height, width)
        sig = 1.0 / (1.0 + jnp.exp(-pre))
        hidden_t = (pre * sig).T.astype(BF16)
        d_pre = (d_hidden * sig * (1.0 + pre * (1.0 - sig))).astype(BF16)
        d_pre_out[t] = d_pre.reshape(height, width, chans)
        for kt in range(3):
            for kh in range(3):
                span = slice(kh * width, (kh + height) * width)
                one = lax.dot_general(
                    vol_rows[t + kt, span, :], d_pre, (((0,), (0,)), ((), ())), preferred_element_type=F32
                )
                two = jnp.dot(hidden_t, cot_rows[t + kt, span, :], preferred_element_type=F32)
                at_one = slice((kt * 3 + kh) * 3 * chans, (kt * 3 + kh + 1) * 3 * chans)
                grads[0, at_one, :] = one if t == 0 else grads[0, at_one, :] + one
                for kw in range(3):
                    block = 26 - (kt * 9 + kh * 3 + kw)
                    at_two = slice(block * chans, (block + 1) * chans)
                    piece = two[:, kw * chans : (kw + 1) * chans]
                    grads[1, at_two, :] = piece if t == 0 else grads[1, at_two, :] + piece
    keep[...] = grads[mine[0]]
    send[...] = grads[1 - mine[0]].astype(BF16)


def back_kernel(mine, cells, prev, nxt, rim, rim_prev, rim_next, weights, out, rows, own_f, prev_f, next_f):
    _, frames, height, width, chans = cells.shape
    load_rim(own_f, rim, 1, mine, height, width)
    load_rim(prev_f, rim_prev, mine[1], mine, height, width)
    load_rim(next_f, rim_next, mine[2], mine, height, width)
    fill_frame(rows, 0, prev, (0, 0), prev_f, (0, 0), height, width, mine[1])
    for t in range(frames):
        fill_frame(rows, t + 1, cells, (0, t), own_f, (0, t), height, width)
    fill_frame(rows, frames + 1, nxt, (0, 0), next_f, (0, 0), height, width, mine[2])
    for t in range(frames):
        total = conv_rows(rows, weights, t, height, width)
        out[t] = total.astype(BF16).reshape(height, width, chans)


def flip_kernel(one, two, one_out, two_out):
    count = one.shape[0]
    for k in range(count):
        one_out[k] = one[count - 1 - k].astype(F32).T.astype(BF16)
        two_out[k] = two[count - 1 - k].astype(F32).T.astype(BF16)


def share_kernel(count, mine, own, *refs):
    received, outs = refs[: len(refs) - count], refs[len(refs) - count :]
    for other in range(count):
        chunk = mine[0] ^ other
        total = own[chunk]
        for part in received:
            total = total + part[chunk].astype(F32)
        outs[other][...] = total.astype(outs[other].dtype)


def merge_kernel(count, inner, places, *refs):
    mine, other, (first, second) = refs[:count], refs[count : 2 * count], refs[2 * count :]
    is_first = places[0] == 0
    for far in range(count):
        for near in range(inner):
            at = (places[1] ^ far) * inner + (places[2] ^ near)
            here = mine[far][near].astype(F32)
            there = other[far][near].astype(F32)
            first[at] = jnp.where(is_first, here, there)
            second[at] = jnp.where(is_first, there, here)


VMEM = pl.BlockSpec(memory_space=pltpu.VMEM)
SMEM = pl.BlockSpec(memory_space=pltpu.SMEM)


def call(kernel, outs, scalars, arrays, scratch=(), name=None):
    return pl.pallas_call(
        kernel,
        out_shape=outs,
        in_specs=[SMEM] * len(scalars) + [VMEM] * len(arrays),
        out_specs=jax.tree.map(lambda _: VMEM, outs),
        scratch_shapes=list(scratch),
        compiler_params=pltpu.CompilerParams(vmem_limit_bytes=VMEM_LIMIT),
        name=name,
    )(*scalars, *arrays)


def shape(dims, dtype):
    return jax.ShapeDtypeStruct(tuple(dims), dtype)


def swap_with(array, mask, devices):
    return lax.ppermute(array, AXES, [(d, d ^ mask) for d in range(devices)])


def body(volume, cotangent, kernel_one, kernel_two):
    frames, height, width, chans = volume.shape
    sizes = {axis: lax.axis_size(axis) for axis in AXES}
    devices = math.prod(sizes.values())
    bits_w, bits_h, bits_t = (sizes[axis].bit_length() - 1 for axis in ("wa", "ha", "ta"))
    pair_bit = bits_w
    far_bits = [bits_w + k for k in range(1, bits_h + bits_t)]
    near_bits = list(range(bits_w))
    here = lax.axis_index(AXES)

    def part_of(bits):
        place = jnp.zeros((), jnp.int32)
        for k, bit in enumerate(bits):
            place = place | (((here >> bit) & 1) << k)
        return place

    def mask_of(bits, number):
        return sum(1 << bit for k, bit in enumerate(bits) if (number >> k) & 1)

    pair, far, near = part_of([pair_bit]), part_of(far_bits), part_of(near_bits)
    far_count, near_count = 1 << len(far_bits), 1 << len(near_bits)

    flat = (27, chans, chans)
    w_back, w_two = call(
        flip_kernel,
        (shape(flat, BF16), shape(flat, BF16)),
        (),
        (kernel_one.reshape(flat), kernel_two.reshape(flat)),
        name="flip",
    )
    by_row = (9, 3 * chans, chans)
    w_one, w_two, w_back = (weights.reshape(by_row) for weights in (kernel_one, w_two, w_back))
    edges = []
    for axis in AXES:
        edges += [lax.axis_index(axis) > 0, lax.axis_index(axis) < sizes[axis] - 1]
    flags = jnp.stack([pair] + [edge.astype(jnp.int32) for edge in edges])

    fields = jnp.stack((volume, cotangent))
    frame_halo = both_ways(*frame_edges(fields), "ta")
    columns = column_halo(fields)
    rim = rim_of(*row_halo(fields, *columns), *columns)
    around = (*frame_halo, rim, *both_ways(*frame_edges(rim), "ta"))
    rim_rows = 2 * height + 4 * width
    patch = pltpu.VMEM((frames + 2, (height + 2) * width, 3 * chans), BF16)
    total_rows = 27 * chans
    d_pre, keep, send = call(
        front_kernel,
        (
            shape(volume.shape, BF16),
            shape((total_rows, chans), F32),
            shape((total_rows, chans), BF16),
        ),
        (flags,),
        (volume, cotangent, *around, w_one, w_two),
        (
            patch,
            patch,
            pltpu.VMEM((2, frames, rim_rows, chans), F32),
            pltpu.VMEM((2, 1, rim_rows, chans), F32),
            pltpu.VMEM((2, 1, rim_rows, chans), F32),
            pltpu.VMEM((2, total_rows, chans), F32),
        ),
        name="front",
    )

    def spread(place, own, received, bits, after):
        count = 1 << len(bits)
        rows = own.shape[0] // count
        split = lambda array: array.reshape(count, rows, chans)
        own, *sends = call(
            functools.partial(share_kernel, count),
            [shape((rows, chans), F32)] + [shape((rows, chans), BF16)] * (count - 1),
            (place.reshape(1),),
            [split(own)] + [split(part) for part in received],
            name="share",
        )
        own, sends, after = lax.optimization_barrier((own, sends, after))
        return own, [swap_with(part, mask_of(bits, m + 1), devices) for m, part in enumerate(sends)], after

    cells = d_pre[None]
    from_pair = swap_with(send, 1 << pair_bit, devices)
    columns = column_halo(cells)
    frame_halo = both_ways(*frame_edges(cells), "ta")
    own, received, columns = spread(far, keep, [from_pair], far_bits, columns)
    lines = row_halo(cells, *columns)
    own, received, lines = spread(near, own, received, near_bits, lines)
    rim = rim_of(*lines, *columns)
    rim_halo = both_ways(*frame_edges(rim), "ta")
    scale = 1.0 / jnp.sqrt(F32(frames * height * width * devices))
    for part in received:
        own = own + part.astype(F32)
    own = (own * scale).astype(BF16)
    own, rim_halo, frame_halo = lax.optimization_barrier((own, rim_halo, frame_halo))

    block = jnp.stack([own] + [swap_with(own, mask_of(near_bits, m), devices) for m in range(1, near_count)])
    block, rim_halo = lax.optimization_barrier((block, rim_halo))
    blocks = [block] + [swap_with(block, mask_of(far_bits, m), devices) for m in range(1, far_count)]
    others = [swap_with(part, 1 << pair_bit, devices) for part in blocks]

    around = (*frame_halo, rim, *rim_halo)
    d_volume = call(
        back_kernel,
        shape(volume.shape, BF16),
        (flags,),
        (cells, *around, w_back),
        (
            patch,
            pltpu.VMEM((1, frames, rim_rows, chans), F32),
            pltpu.VMEM((1, 1, rim_rows, chans), F32),
            pltpu.VMEM((1, 1, rim_rows, chans), F32),
        ),
        name="back",
    )
    grad_shape = shape((far_count * near_count, own.shape[0], chans), F32)
    grad_one, grad_two = call(
        functools.partial(merge_kernel, far_count, near_count),
        (grad_shape, grad_shape),
        (jnp.stack((pair, far, near)),),
        (*blocks, *others),
        name="merge",
    )
    return d_volume, grad_one.reshape(kernel_one.shape), grad_two.reshape(kernel_two.shape)


def solution(mesh):
    spec = P("ta", "ha", "wa", None)
    return jax.shard_map(
        body, mesh=mesh, in_specs=(spec, spec, P(), P()), out_specs=(spec, P(), P()), check_vma=False
    )
```
